256 devices in a mesh: week: 32 (over z, y), seg: 8 (over x, core).
Axes of the slice: x: 4, y: 4, z: 8, core: 2. Of those that a mesh axis runs over, the one named last changes fastest.
Arguments:
- right_side: float32 [48, 8, 8192], P(None, 'seg', 'week'), may hold values from -6 to 6
- jacobians: bfloat16 [256, 256, 4096], P('week', None, 'seg'), may hold values from -0.09375 to 0.09375
- week_blocks: int32 [256, 32], P('week', 'seg'), may hold values from 0 to 63, as said below
- block_kind: int32 [8, 64], P('seg', 'week'), may hold values from 0 to 7
- diagonal_table: float32 [8, 128, 128], replicated, as said below
- precond_table: float32 [8, 128, 128], replicated, as said below
Outputs:
- solution_field: float32 [48, 8, 8192], P(None, 'seg', 'week')
- residual: float32 [48, 8, 8192], P(None, 'seg', 'week')
The draws below stay inside these ranges and needn't reach their ends.
Inputs may be any that keep to these rules, and one draw needn't show every extreme that they name: `week_blocks`: entry j of a week's row names a block of segment j // 4 by its number within that segment; the 4 entries of one segment in one row are distinct. `diagonal_table`: each block is symmetric positive definite. `precond_table`: each block is symmetric positive definite.
All inputs are finite; a program needn't handle non-finite values.
Results may differ from the reference program's by a relative error of at most 0.035.
Values may be sent and summed in bfloat16 or wider, within the bound.
No kernel may reach another device: no remote copies, remote signals or barrier semaphores. Data moves between devices by JAX's collectives and lax.ppermute only.
A program may use at most 64 MiB of HBM per device.

```python
import math
import jax
import jax.numpy as jnp
from jax import lax

P_SIZE = 65536
S = 4096
R = 256
BLK = 128
KINDS = 8
ITERS = 4
NRHS = 48
W_DEV = 8
WEEKS = 256
SEGS = 8
SEG_LEN = 8192
SUB_SEG = 512
KB = 4
BLOCKS_SEG = 64


def draw_week_blocks(key, part):
    scores = jax.random.randint(key, (WEEKS, SEGS, BLOCKS_SEG), 0, 1 << 20) * BLOCKS_SEG + jnp.arange(BLOCKS_SEG, dtype=jnp.int32)
    picked = jnp.argsort(scores, axis=-1, stable=True)[:, :, :KB]
    return picked.reshape(WEEKS, SEGS * KB).astype(jnp.int32)


def symmetric_blocks(key, lower, upper):
    key_one, key_two = jax.random.split(key)
    diagonal_part = jax.random.uniform(key_one, (KINDS, BLK), jnp.float32, lower, upper)
    random_part = jax.random.normal(key_two, (KINDS, BLK, BLK), jnp.float32) * (0.5 / math.sqrt(2.0 * BLK))
    symmetric = random_part + jnp.swapaxes(random_part, 1, 2)
    return symmetric + diagonal_part[:, :, None] * jnp.eye(BLK, dtype=jnp.float32)


def draw_diagonal_table(key, part):
    return symmetric_blocks(jax.random.fold_in(key, 11), 1.5, 2.5)


def draw_precond_table(key, part):
    return symmetric_blocks(jax.random.fold_in(key, 23), 1.5, 3.0)


def place_ends(drawn, key, smallest, high):
    place = [jax.random.randint(jax.random.fold_in(key, axis), (), 0, length) for axis, length in enumerate(drawn.shape)]
    main_axis = drawn.shape.index(max(drawn.shape))
    neighbour = place[:main_axis] + [(place[main_axis] + 1) % drawn.shape[main_axis]] + place[main_axis + 1:]
    return drawn.at[tuple(place)].set(smallest).at[tuple(neighbour)].set(high)


def steps_of(key, extent, cuts, smallest, high):
    factor_of, own = 1.0, jax.random.fold_in(key, 6)
    for position, parts in cuts:
        steps = jnp.exp(jax.random.uniform(jax.random.fold_in(own, position), (parts,), jnp.float32, smallest / len(cuts), high / len(cuts)))
        factor_of = factor_of * jnp.repeat(steps, extent[position] // parts).reshape([-1 if axis == position else 1 for axis in range(len(extent))])
    return factor_of


def bell_draw(own_key, extent, deviation, reach, cuts=(), kind=jnp.bfloat16):
    values = jax.random.normal(own_key, extent, jnp.float32) * deviation
    if len(cuts) > 0:
        values = steps_of(own_key, extent, cuts, -0.22, 0.18) * values
    return jnp.clip(values, min=-reach, max=reach).astype(kind)


def setup_inputs(seed: int = 0) -> dict:
    keys = jax.random.split(jax.random.key(seed), 7)
    return {
        "right_side": bell_draw(keys[0], (NRHS, SEGS, SEG_LEN), 1.0, 6.0, ((1, 8), (2, 32)), jnp.float32),
        "jacobians": bell_draw(keys[1], (WEEKS, R, S), (max(R * WEEKS * SUB_SEG // SEG_LEN, 1)) ** -0.5, 0.09375, ((0, 32), (2, 8))),
        "week_blocks": draw_week_blocks(jax.random.fold_in(keys[6], 71), 0),
        "block_kind": place_ends(jax.random.randint(keys[3], (SEGS, BLOCKS_SEG), 0, KINDS), jax.random.fold_in(keys[3], 1), 0, KINDS - 1).astype(jnp.int32),
        "diagonal_table": draw_diagonal_table(jax.random.fold_in(keys[6], 71), 0),
        "precond_table": draw_precond_table(jax.random.fold_in(keys[6], 71), 0),
    }


def block_apply(vector, blocks):
    shaped = vector.reshape(vector.shape[0], blocks.shape[0], blocks.shape[1])
    result = jnp.einsum("kbc,bcd->kbd", shaped, blocks, precision=lax.Precision.HIGHEST)
    return result.reshape(vector.shape[0], -1)


def reference(right_side, jacobians, week_blocks, block_kind, diagonal_table, precond_table):
    right = right_side.reshape(NRHS, P_SIZE)
    kinds = block_kind.reshape(-1)
    diag_blocks = diagonal_table[kinds]
    pre_blocks = precond_table[kinds]
    column = jnp.arange(S, dtype=jnp.int32)
    columns = ((column // SUB_SEG) * SEG_LEN + week_blocks[:, column // BLK] * BLK + column % BLK).astype(jnp.int32)
    stacked = jacobians.reshape(WEEKS // W_DEV, W_DEV, R, S)
    index_blocks = columns.reshape(WEEKS // W_DEV, W_DEV, S)

    def operate(direction):
        rounded = direction.astype(jnp.bfloat16).astype(jnp.float32)

        def add_weeks(total_acc, pieces):
            factor, cols_here = pieces
            factor32 = factor.astype(jnp.float32)
            picked = rounded[:, cols_here]
            projected = jnp.einsum("wrc,kwc->kwr", factor32, picked, precision=lax.Precision.HIGHEST)
            projected = lax.optimization_barrier(projected.astype(jnp.bfloat16)).astype(jnp.float32)
            spread = jnp.einsum("wrc,kwr->kwc", factor32, projected, precision=lax.Precision.HIGHEST)
            return total_acc.at[:, cols_here].add(spread), None

        image, _ = lax.scan(add_weeks, jnp.zeros((NRHS, P_SIZE), jnp.float32), (stacked, index_blocks))
        return image + block_apply(direction, diag_blocks)

    def inner(first_vec, second_vec):
        return jnp.sum(first_vec * second_vec, axis=1)

    solution = jnp.zeros((NRHS, P_SIZE), jnp.float32)
    residual = right
    precond = block_apply(residual, pre_blocks)
    direction = precond
    rz_now = inner(residual, precond)
    for step in range(ITERS):
        image = operate(direction)
        step_size = rz_now / inner(direction, image)
        solution = solution + step_size[:, None] * direction
        residual = residual - step_size[:, None] * image
        if step + 1 < ITERS:
            precond = block_apply(residual, pre_blocks)
            rz_next = inner(residual, precond)
            direction = precond + (rz_next / rz_now)[:, None] * direction
            rz_now = rz_next
    return solution.reshape(NRHS, SEGS, SEG_LEN), residual.reshape(NRHS, SEGS, SEG_LEN)
```

```python
import jax
import jax.numpy as jnp
from jax import lax
from jax.sharding import Mesh
from jax.sharding import PartitionSpec as P

ITERS = 4
SEG = ("seg_0", "seg_1")
WEEK = ("week_0", "week_1")
Z, Y, X, CORE = "week_0", "week_1", "seg_0", "seg_1"
BF16 = jnp.bfloat16
F32 = jnp.float32
LANES = 128
GROUP = 8
KEYS = 16


def ring(axis, shift):
    size = lax.axis_size(axis)
    return [(place, (place + shift) % size) for place in range(size)]


def shifted(array, axis, shift):
    return lax.ppermute(array, axis, ring(axis, shift))


def from_ring(array, axis):
    return [array] + [shifted(array, axis, k) for k in range(1, lax.axis_size(axis))]


def exchange(array, axis):
    return lax.all_to_all(array, axis, 0, 0, tiled=True)


def three_parts(values):
    high = values.astype(BF16).astype(F32)
    rest = values - high
    middle = rest.astype(BF16).astype(F32)
    return jnp.stack([high, middle, rest - middle])


def scalar_tile(values):
    kinds, rows = values.shape
    parts = jnp.moveaxis(three_parts(values), 0, 1).reshape(kinds * 3, rows // GROUP, GROUP)
    parts = jnp.pad(jnp.transpose(parts, (2, 1, 0)), ((0, 0), (0, 0), (0, KEYS - kinds * 3)))
    tile = parts.reshape(GROUP, -1)
    return jnp.pad(tile, ((0, 0), (0, LANES - tile.shape[1]))).astype(BF16)[None]


def tile_sums(tiles, kinds, rows):
    total = tiles.astype(F32).reshape(-1, GROUP, LANES).sum(axis=0)
    total = total[:, : rows // GROUP * KEYS].reshape(GROUP, rows // GROUP, KEYS)
    total = total[:, :, : kinds * 3].reshape(GROUP, rows // GROUP, kinds, 3).sum(axis=3)
    return jnp.transpose(total, (2, 1, 0)).reshape(kinds, rows)


def block_apply(vector, blocks):
    return jnp.einsum("bkc,bcd->bkd", vector, blocks, precision=lax.Precision.HIGHEST)


def dots(first, second):
    return jnp.sum(first * second, axis=(0, 2))


def per_device(right_side, jacobians, week_blocks, block_kind, diagonal_table, precond_table):
    rhs_all = right_side.shape[0]
    rows = rhs_all // 2
    week_count, rank_count, columns = jacobians.shape
    picks = week_blocks.shape[1]
    own_blocks = right_side.shape[2] // LANES
    z_size, y_size, x_size = (lax.axis_size(axis) for axis in (Z, Y, X))
    here_y = lax.axis_index(Y)
    core = lax.axis_index(CORE)

    def both(own):
        return jnp.stack([own, shifted(own, CORE, 1)])

    right = right_side[:, 0, :].reshape(2, rows, own_blocks, LANES)
    right = jnp.transpose(right, (0, 2, 1, 3))
    kept = jnp.where(core == 0, right[0], right[1])
    given = jnp.where(core == 0, right[1], right[0])
    right = jnp.concatenate([kept, shifted(given, CORE, 1)])
    factors = both(jacobians)
    factors = jnp.transpose(factors, (1, 2, 0, 3)).reshape(week_count, rank_count, 2 * columns)
    small = both(jnp.concatenate([week_blocks.reshape(-1), block_kind.reshape(-1)]))
    ids = jnp.transpose(small[:, : week_count * picks].reshape(2, week_count, picks), (1, 0, 2))
    kinds = small[:, week_count * picks :].reshape(-1)
    diag_blocks = diagonal_table[kinds]
    pre_blocks = precond_table[kinds]
    held = 2 * own_blocks
    tiles = held * rows // GROUP

    owner = ids // own_blocks
    place = ids % own_blocks + own_blocks * jnp.arange(2, dtype=jnp.int32)[None, :, None]
    owner_z, owner_y = owner // y_size, owner % y_size
    from_y = (here_y - owner_y) % y_size
    to_y = (owner_y - here_y) % y_size
    pick_at = ((from_y * z_size + owner_z) * held + place).reshape(-1)
    put_at = ((to_y * z_size + owner_z) * held + place).reshape(-1)
    slots = y_size * z_size * held
    onehot = (put_at[:, None] == jnp.arange(slots, dtype=jnp.int32)[None, :]).astype(F32)

    def operate(vector, scalars):
        piece = jnp.concatenate(
            [vector.astype(BF16).reshape(tiles, GROUP, LANES), scalar_tile(scalars)]
        )
        along_z = exchange(jnp.broadcast_to(piece[None], (z_size, *piece.shape)), Z)
        gathered = jnp.stack(from_ring(along_z, Y))
        column_sums = tile_sums(gathered[:, :, tiles], scalars.shape[0], rows)
        blocks = gathered[:, :, :tiles].reshape(slots, rows, LANES)
        picked = jnp.take(blocks, pick_at, axis=0, mode="clip")
        picked = picked.reshape(week_count, 2 * picks, rows, LANES)
        picked = jnp.moveaxis(picked, 2, 1).reshape(week_count, rows, 2 * columns)
        partial = jnp.einsum("wkc,wrc->wkr", picked, factors, preferred_element_type=F32)
        partial = jnp.concatenate(
            [partial.astype(BF16).reshape(-1, GROUP, LANES), scalar_tile(column_sums)]
        )
        arrived = jnp.stack(from_ring(partial, X))
        totals = tile_sums(arrived[:, -1], scalars.shape[0], rows)
        projected = arrived[:, :-1].astype(F32).sum(axis=0)
        projected = projected.reshape(week_count, rows, rank_count).astype(BF16)
        energy = jnp.sum(jnp.square(projected.astype(F32)), axis=(0, 2))
        spread = jnp.einsum("wkr,wrc->wkc", projected, factors, preferred_element_type=F32)
        spread = spread.reshape(week_count, rows, 2 * picks, LANES)
        spread = jnp.moveaxis(spread, 2, 1).reshape(-1, rows, LANES)
        placed = jnp.einsum("bs,bkc->skc", onehot, spread, precision=lax.Precision.HIGHEST)
        placed = placed.astype(BF16).reshape(y_size, z_size, tiles, GROUP, LANES)
        tile = scalar_tile(energy[None])
        tile = jnp.broadcast_to(tile, (y_size, z_size, *tile.shape))
        placed = jnp.concatenate([placed, tile], axis=2)
        arrived = jnp.stack(
            [placed[0]] + [shifted(placed[k], Y, k) for k in range(1, y_size)]
        )
        energy = tile_sums(arrived[:, 0, tiles], 1, rows)
        terms = arrived[:, :, :tiles].astype(F32).sum(axis=0).astype(BF16)
        tile = jnp.broadcast_to(scalar_tile(energy), (z_size, 1, GROUP, LANES))
        arrived = exchange(jnp.concatenate([terms, tile], axis=1), Z)
        energy = tile_sums(arrived[:, tiles], 1, rows)[0]
        image = arrived[:, :tiles].astype(F32).sum(axis=0).reshape(held, rows, LANES)
        return image, totals, energy

    residual = right
    solution = jnp.zeros_like(right)
    direction = image = None
    for step in range(ITERS):
        precond = block_apply(residual, pre_blocks)
        diagonal = block_apply(precond, diag_blocks)
        scalars = [dots(residual, precond), dots(precond, diagonal)]
        if step:
            scalars.append(dots(precond, image))
        applied, totals, energy = operate(precond, jnp.stack(scalars))
        applied = applied + diagonal
        curvature = energy + totals[1]
        if step:
            beta = totals[0] / rz_now
            curvature = curvature + 2 * beta * totals[2] + beta * beta * bent
            direction = precond + beta[None, :, None] * direction
            image = applied + beta[None, :, None] * image
        else:
            direction, image = precond, applied
        rz_now, bent = totals[0], curvature
        step_size = (rz_now / bent)[None, :, None]
        solution = solution + step_size * direction
        residual = residual - step_size * image

    results = jnp.stack([solution, residual])
    other = shifted(results[:, own_blocks:], CORE, 1)
    own = results[:, :own_blocks]
    first = jnp.where(core == 0, own, other)
    second = jnp.where(core == 0, other, own)
    results = jnp.stack([first, second], axis=1)
    results = jnp.transpose(results, (0, 1, 3, 2, 4)).reshape(2, rhs_all, 1, -1)
    return (results[0], results[1])


def solution(mesh):
    torus = Mesh(mesh.devices.reshape(8, 4, 4, 2), ("week_0", "week_1", "seg_0", "seg_1"))
    return jax.shard_map(
        per_device,
        mesh=torus,
        in_specs=(P(None, SEG, WEEK), P(WEEK, None, SEG), P(WEEK, SEG), P(SEG, WEEK), P(), P()),
        out_specs=(P(None, SEG, WEEK), P(None, SEG, WEEK)),
        check_vma=False,
    )
```

```python
import functools

import jax
import jax.numpy as jnp
from jax import lax
from jax.experimental import pallas as pl
from jax.experimental.pallas import tpu as pltpu
from jax.sharding import Mesh
from jax.sharding import PartitionSpec as P

ITERS = 4
UNROLL = False
SEG = ("seg_0", "seg_1")
WEEK = ("week_0", "week_1")
Z, Y, X, CORE = "week_0", "week_1", "seg_0", "seg_1"
BF16 = jnp.bfloat16
F32 = jnp.float32
LANES = 128
GROUP = 8
KEYS = 16
VMEM = pl.BlockSpec(memory_space=pltpu.VMEM)
SMEM = pl.BlockSpec(memory_space=pltpu.SMEM)


def ring(axis, shift):
    size = lax.axis_size(axis)
    return [(place, (place + shift) % size) for place in range(size)]


def shifted(array, axis, shift):
    return lax.ppermute(array, axis, ring(axis, shift))


def from_ring(array, axis):
    return [array] + [shifted(array, axis, k) for k in range(1, lax.axis_size(axis))]


def exchange(array, axis):
    return lax.all_to_all(array, axis, 0, 0, tiled=True)


def lanes():
    return lax.broadcasted_iota(jnp.int32, (GROUP, LANES), 1)


def whole(tile):
    return tile + pltpu.roll(tile, LANES - 1, 1) + pltpu.roll(tile, LANES - 2, 1)


def in_parts(values):
    high = values.astype(BF16).astype(F32)
    rest = values - high
    middle = rest.astype(BF16).astype(F32)
    return (high + pltpu.roll(middle, 1, 1) + pltpu.roll(rest - middle, 2, 1)).astype(BF16)


def firsts(tile, kinds, groups):
    lane = lanes()
    keep = (lane % KEYS % 3 == 0) & (lane % KEYS < 3 * kinds) & (lane < groups * KEYS)
    return jnp.where(keep, tile, 0.0)


def in_tile(columns):
    lane = lanes()
    tile = jnp.zeros((GROUP, LANES), F32)
    for (group, kind), column in columns.items():
        tile = jnp.where(lane == group * KEYS + 3 * kind, column, tile)
    return tile


def total_of(refs_and_places):
    total = None
    for ref, place in refs_and_places:
        value = ref[place].astype(F32)
        total = value if total is None else total + value
    return total


def project(groups, tiles, picks, at_ref, part_ref, got, near, far, out):
    weeks, rank, columns = near.shape
    rows = groups * GROUP
    each = picks // 2
    for week in range(weeks):
        total = None
        for side, factor in enumerate((near, far)):
            blocks = []
            for pick in range(each):
                number = week * picks + side * each + pick
                block = got[at_ref[number], pl.ds(part_ref[number], groups)]
                blocks.append(block.astype(F32).reshape(rows, LANES).astype(BF16))
            term = lax.dot_general(
                jnp.concatenate(blocks, axis=1),
                factor[week],
                (((1,), (1,)), ((), ())),
                preferred_element_type=F32,
            )
            total = term if total is None else total + term
        for half in range(rank // LANES):
            piece = total[:, half * LANES : (half + 1) * LANES].reshape(groups, GROUP, LANES)
            first = (week * (rank // LANES) + half) * groups
            out[first : first + groups] = piece.astype(BF16)
    sums = total_of([(got, (place, tiles)) for place in range(got.shape[0])])
    out[out.shape[0] - 1] = in_parts(firsts(whole(sums), 3, groups))


def spread(groups, tiles, picks, at_ref, *refs):
    count = len(refs) // 2 - 2
    parts, (near, far) = refs[:count], refs[count : count + 2]
    outs, totals, sums = refs[count + 2 : 2 * count + 2], refs[-2], refs[-1]
    weeks, rank, columns = near.shape
    rows = groups * GROUP
    each = picks // 2
    halves = rank // LANES
    last = parts[0].shape[0] - 1
    totals[...] = firsts(whole(total_of([(part, last) for part in parts])), 3, groups)
    sums[...] = jnp.zeros_like(sums)
    energy = jnp.zeros((groups, GROUP, LANES), F32)
    for week in range(weeks):
        pieces = []
        for half in range(halves):
            first = (week * halves + half) * groups
            piece = total_of([(part, slice(first, first + groups)) for part in parts])
            energy = energy + piece * piece
            pieces.append(piece.reshape(rows, LANES).astype(BF16))
        projected = jnp.concatenate(pieces, axis=1)
        for side, factor in enumerate((near, far)):
            term = jnp.dot(projected, factor[week], preferred_element_type=F32)
            for pick in range(each):
                place = at_ref[week * picks + side * each + pick]
                block = term[:, pick * LANES : (pick + 1) * LANES]
                sums[place] = sums[place] + block.reshape(groups, GROUP, LANES)
    columns = {}
    for group in range(groups):
        columns[group, 0] = jnp.sum(energy[group], axis=1, keepdims=True)
    tile = in_parts(in_tile(columns))
    depth = outs[0].shape[0]
    held = tiles // groups
    for k, out in enumerate(outs):
        for place in range(depth):
            for block in range(held):
                value = sums[(k * depth + place) * held + block]
                out[place, block * groups : (block + 1) * groups] = value.astype(out.dtype)
            out[place, tiles] = tile.astype(out.dtype)


def add_up(groups, tiles, *refs):
    arrived, out = refs[:-1], refs[-1]
    for place in range(out.shape[0]):
        value = total_of([(ref, (place, slice(0, tiles))) for ref in arrived])
        out[place, 0:tiles] = value.astype(BF16)
        sums = total_of([(ref, (place, tiles)) for ref in arrived])
        out[place, tiles] = in_parts(firsts(whole(sums), 1, groups))


def prepare(groups, tiles, kinds, diag_table, pre_table, residual, image, sent, precond, diagonal):
    held = tiles // groups
    rows = groups * GROUP
    shape = (groups, GROUP, LANES)
    dots = [None] * 3
    for block in range(held):
        kind = kinds[block]
        left = residual[block]
        value = jnp.dot(
            left.reshape(rows, LANES), pre_table[kind],
            precision=lax.Precision.HIGHEST, preferred_element_type=F32,
        )
        scaled = jnp.dot(
            value, diag_table[kind],
            precision=lax.Precision.HIGHEST, preferred_element_type=F32,
        ).reshape(shape)
        value = value.reshape(shape)
        precond[block] = value
        diagonal[block] = scaled
        for place in range(sent.shape[0]):
            sent[place, block * groups : (block + 1) * groups] = value.astype(BF16)
        terms = [left * value, value * scaled]
        if image is not None:
            terms.append(value * image[block])
        for kind, term in enumerate(terms):
            dots[kind] = term if dots[kind] is None else dots[kind] + term
    columns = {}
    for kind, dot in enumerate(dots):
        if dot is not None:
            for group in range(groups):
                columns[group, kind] = jnp.sum(dot[group], axis=1, keepdims=True)
    tile = in_parts(in_tile(columns))
    for place in range(sent.shape[0]):
        sent[place, tiles] = tile


def begin(groups, tiles, kinds, diag_table, pre_table, residual, sent, precond, diagonal):
    prepare(
        groups, tiles, kinds, diag_table, pre_table, residual, None, sent, precond, diagonal
    )


def update(groups, tiles, more, kinds, diag_table, pre_table, arrived, totals, carry, *refs):
    precond, diagonal, direction, image, answer, residual = refs[:6]
    if more:
        sent, new_carry, new_precond, new_diagonal = refs[6:10]
        new_direction, new_image, new_answer, new_residual = refs[10:]
    else:
        new_answer, new_residual = refs[6:]
    held = tiles // groups
    depth = arrived.shape[0]
    energies = whole(total_of([(arrived, (place, tiles)) for place in range(depth)]))
    sums, before = totals[...], carry[...]
    columns = {}
    for group in range(groups):

        def column(tile, kind):
            lane = group * KEYS + 3 * kind
            return tile[:, lane : lane + 1]

        now = column(sums, 0)
        beta = now / column(before, 0)
        bent = column(energies, 0) + column(sums, 1)
        bent = bent + 2.0 * beta * column(sums, 2) + beta * beta * column(before, 1)
        step = now / bent
        columns[group, 0], columns[group, 1] = now, bent
        for block in range(held):
            tile = block * groups + group
            applied = total_of([(arrived, (place, tile)) for place in range(depth)])
            applied = applied + diagonal[block, group]
            heading = precond[block, group] + beta * direction[block, group]
            applied = applied + beta * image[block, group]
            if more:
                new_direction[block, group] = heading
                new_image[block, group] = applied
            new_answer[block, group] = answer[block, group] + step * heading
            new_residual[block, group] = residual[block, group] - step * applied
    if more:
        new_carry[...] = in_tile(columns)
        prepare(
            groups, tiles, kinds, diag_table, pre_table, new_residual, new_image,
            sent, new_precond, new_diagonal,
        )


def call(body, shapes, operands, smem, name, flops, scratch=()):
    return pl.pallas_call(
        body,
        out_shape=shapes,
        in_specs=[SMEM] * smem + [VMEM] * (len(operands) - smem),
        out_specs=jax.tree.map(lambda _: VMEM, shapes),
        scratch_shapes=list(scratch),
        compiler_params=pltpu.CompilerParams(vmem_limit_bytes=32 * 1024 * 1024),
        cost_estimate=pl.CostEstimate(flops=flops, bytes_accessed=1 << 20, transcendentals=0),
        name=name,
    )(*operands)


def per_device(right_side, jacobians, week_blocks, block_kind, diagonal_table, precond_table):
    rhs_all = right_side.shape[0]
    rows = rhs_all // 2
    groups = rows // GROUP
    week_count, rank_count, columns = jacobians.shape
    picks = 2 * week_blocks.shape[1]
    own_blocks = right_side.shape[2] // LANES
    z_size, y_size, x_size = (lax.axis_size(axis) for axis in (Z, Y, X))
    here_y = lax.axis_index(Y)
    core = lax.axis_index(CORE)
    held = 2 * own_blocks
    tiles = held * groups
    shape = jax.ShapeDtypeStruct

    other_jacobians = shifted(jacobians, CORE, 1)
    right = right_side[:, 0, :].reshape(2, rows, own_blocks, LANES)
    right = jnp.transpose(right, (0, 2, 1, 3))
    kept = jnp.where(core == 0, right[0], right[1])
    given = jnp.where(core == 0, right[1], right[0])
    right = jnp.concatenate([kept, shifted(given, CORE, 1)])
    right = right.reshape(held, groups, GROUP, LANES)
    small = jnp.concatenate([week_blocks.reshape(-1), block_kind.reshape(-1)])
    small = jnp.stack([small, shifted(small, CORE, 1)])
    ids = small[:, : week_blocks.size].reshape(2, week_count, picks // 2)
    ids = jnp.transpose(ids, (1, 0, 2))
    kinds = small[:, week_blocks.size :].reshape(-1)

    owner = ids // own_blocks
    place = ids % own_blocks + own_blocks * jnp.arange(2, dtype=jnp.int32)[None, :, None]
    owner_z, owner_y = owner // y_size, owner % y_size
    pick_at = (((here_y - owner_y) % y_size) * z_size + owner_z).reshape(-1)
    pick_part = (place * groups).reshape(-1)
    put_at = ((((owner_y - here_y) % y_size) * z_size + owner_z) * held + place).reshape(-1)

    vector = shape((held, groups, GROUP, LANES), F32)
    tile = shape((GROUP, LANES), F32)
    sent_shape = shape((z_size, tiles + 1, GROUP, LANES), BF16)
    part_shape = shape((week_count * rank_count // LANES * groups + 1, GROUP, LANES), BF16)
    big_flops = 2 * week_count * rank_count * columns * 2 * rows
    slots = y_size * z_size * held
    tables = (kinds, diagonal_table, precond_table)

    def operate(sent):
        along_z = exchange(sent, Z)
        got = jnp.concatenate(from_ring(along_z, Y))
        partial = call(
            functools.partial(project, groups, tiles, picks),
            part_shape,
            (pick_at, pick_part, got, jacobians, other_jacobians),
            2, "project", big_flops,
        )
        own = shape(sent_shape.shape, F32)
        *terms, totals = call(
            functools.partial(spread, groups, tiles, picks),
            (own, *[sent_shape] * (y_size - 1), tile),
            (put_at, *from_ring(partial, X), jacobians, other_jacobians),
            1, "spread", big_flops,
            scratch=[pltpu.VMEM((slots, groups, GROUP, LANES), F32)],
        )
        terms = [terms[0]] + [shifted(terms[k], Y, k) for k in range(1, y_size)]
        summed = call(
            functools.partial(add_up, groups, tiles), sent_shape, tuple(terms), 0, "add_up", 1 << 20
        )
        return exchange(summed, Z), totals

    sent, precond, diagonal = call(
        functools.partial(begin, groups, tiles),
        (sent_shape, vector, vector),
        (*tables, right),
        1, "begin", 1 << 22,
    )
    zeros = jnp.zeros(vector.shape, F32)
    carry = jnp.full(tile.shape, jnp.inf, F32)
    carry = jnp.where(jnp.arange(LANES)[None, :] % KEYS == 0, carry, 0.0)
    state = (sent, carry, precond, diagonal, zeros, zeros, zeros, right)

    def advance(step, state, more):
        sent, carry, *vectors = state
        arrived, totals = operate(sent)
        shapes = (vector, vector)
        if more:
            shapes = (sent_shape, tile, *[vector] * 6)
        return tuple(
            call(
                functools.partial(update, groups, tiles, more),
                shapes,
                (*tables, arrived, totals, carry, *vectors),
                1, "update", 1 << 22,
            )
        )

    if UNROLL:
        for step in range(ITERS):
            state = advance(step, state, step + 1 < ITERS)
        answer, residual = state
    else:
        state = lax.fori_loop(0, ITERS - 1, lambda step, now: advance(step, now, True), state)
        answer, residual = advance(ITERS - 1, state, False)

    results = jnp.stack([answer, residual]).reshape(2, held, rows, LANES)
    other = shifted(results[:, own_blocks:], CORE, 1)
    own = results[:, :own_blocks]
    first = jnp.where(core == 0, own, other)
    second = jnp.where(core == 0, other, own)
    results = jnp.stack([first, second], axis=1)
    results = jnp.transpose(results, (0, 1, 3, 2, 4)).reshape(2, rhs_all, 1, -1)
    return (results[0], results[1])


def solution(mesh):
    torus = Mesh(mesh.devices.reshape(8, 4, 4, 2), ("week_0", "week_1", "seg_0", "seg_1"))
    return jax.shard_map(
        per_device,
        mesh=torus,
        in_specs=(P(None, SEG, WEEK), P(WEEK, None, SEG), P(WEEK, SEG), P(SEG, WEEK), P(), P()),
        out_specs=(P(None, SEG, WEEK), P(None, SEG, WEEK)),
        check_vma=False,
    )
```

```python
import functools

import jax
import jax.numpy as jnp
from jax import lax
from jax.experimental import pallas as pl
from jax.experimental.pallas import tpu as pltpu
from jax.sharding import Mesh
from jax.sharding import PartitionSpec as P

ITERS = 4
SEG = ("seg_0", "seg_1")
WEEK = ("week_0", "week_1")
Z, Y, X, CORE = "week_0", "week_1", "seg_0", "seg_1"
BF16 = jnp.bfloat16
F32 = jnp.float32
LANES = 128
GROUP = 8
KEYS = 16
VMEM = pl.BlockSpec(memory_space=pltpu.VMEM)
SMEM = pl.BlockSpec(memory_space=pltpu.SMEM)


def ring(axis, shift):
    size = lax.axis_size(axis)
    return [(place, (place + shift) % size) for place in range(size)]


def shifted(array, axis, shift):
    return lax.ppermute(array, axis, ring(axis, shift))


def by_distance(size):
    return sorted(range(1, size), key=lambda k: (min(k, size - k), k))


def from_ring(array, axis):
    size = lax.axis_size(axis)
    moved = {0: array}
    for k in by_distance(size):
        moved[k] = shifted(array, axis, k)
    return [moved[k] for k in range(size)]


def exchange(array, axis):
    return lax.all_to_all(array, axis, 0, 0, tiled=True)


def lanes():
    return lax.broadcasted_iota(jnp.int32, (GROUP, LANES), 1)


def whole(tile):
    return tile + pltpu.roll(tile, LANES - 1, 1) + pltpu.roll(tile, LANES - 2, 1)


def in_parts(values):
    high = values.astype(BF16).astype(F32)
    rest = values - high
    middle = rest.astype(BF16).astype(F32)
    return (high + pltpu.roll(middle, 1, 1) + pltpu.roll(rest - middle, 2, 1)).astype(BF16)


def firsts(tile, kinds, groups):
    lane = lanes()
    keep = (lane % KEYS % 3 == 0) & (lane % KEYS < 3 * kinds) & (lane < groups * KEYS)
    return jnp.where(keep, tile, 0.0)


def in_tile(columns):
    lane = lanes()
    tile = jnp.zeros((GROUP, LANES), F32)
    for (group, kind), column in columns.items():
        tile = jnp.where(lane == group * KEYS + 3 * kind, column, tile)
    return tile


def total_of(refs_and_places):
    total = None
    for ref, place in refs_and_places:
        value = ref[place].astype(F32)
        total = value if total is None else total + value
    return total


def project(groups, tiles, picks, at_ref, got, near, far, out):
    weeks, rank, columns = near.shape
    rows = groups * GROUP
    each = picks // 2
    for week in range(weeks):
        total = None
        for side, factor in enumerate((near, far)):
            blocks = []
            for pick in range(each):
                number = week * picks + side * each + pick
                block = got[pl.ds(at_ref[number], groups)]
                blocks.append(block.astype(F32).reshape(rows, LANES).astype(BF16))
            term = lax.dot_general(
                jnp.concatenate(blocks, axis=1),
                factor[week],
                (((1,), (1,)), ((), ())),
                preferred_element_type=F32,
            )
            total = term if total is None else total + term
        for half in range(rank // LANES):
            piece = total[:, half * LANES : (half + 1) * LANES].reshape(groups, GROUP, LANES)
            first = (week * (rank // LANES) + half) * groups
            out[first : first + groups] = piece.astype(BF16)
    sums = total_of([(got, place) for place in range(tiles, got.shape[0], tiles + 1)])
    out[out.shape[0] - 1] = in_parts(firsts(whole(sums), 3, groups))


def spread(groups, tiles, picks, at_ref, *refs):
    count = len(refs) // 2 - 2
    parts, (near, far) = refs[:count], refs[count : count + 2]
    outs, totals, sums = refs[count + 2 : 2 * count + 2], refs[-2], refs[-1]
    weeks, rank, columns = near.shape
    rows = groups * GROUP
    each = picks // 2
    halves = rank // LANES
    last = parts[0].shape[0] - 1
    totals[...] = firsts(whole(total_of([(part, last) for part in parts])), 3, groups)
    sums[...] = jnp.zeros_like(sums)
    energy = jnp.zeros((groups, GROUP, LANES), F32)
    for week in range(weeks):
        pieces = []
        for half in range(halves):
            first = (week * halves + half) * groups
            piece = total_of([(part, slice(first, first + groups)) for part in parts])
            energy = energy + piece * piece
            pieces.append(piece.reshape(rows, LANES).astype(BF16))
        projected = jnp.concatenate(pieces, axis=1)
        for side, factor in enumerate((near, far)):
            term = jnp.dot(projected, factor[week], preferred_element_type=F32)
            for pick in range(each):
                place = at_ref[week * picks + side * each + pick]
                block = term[:, pick * LANES : (pick + 1) * LANES]
                sums[place] = sums[place] + block.reshape(groups, GROUP, LANES)
    columns = {}
    for group in range(groups):
        columns[group, 0] = jnp.sum(energy[group], axis=1, keepdims=True)
    tile = in_parts(in_tile(columns))
    blocks = outs[0].shape[0] // groups
    for k, out in enumerate(outs):
        for block in range(blocks):
            value = sums[k * blocks + block]
            out[block * groups : (block + 1) * groups] = value.astype(out.dtype)
        out[blocks * groups] = tile.astype(out.dtype)


def add_up(groups, tiles, *refs):
    arrived, out = refs[:-1], refs[-1]
    depth = out.shape[0]
    sums = total_of([(ref, depth * tiles) for ref in arrived])
    tile = in_parts(firsts(whole(sums), 1, groups))
    for place in range(depth):
        span = slice(place * tiles, (place + 1) * tiles)
        out[place, 0:tiles] = total_of([(ref, span) for ref in arrived]).astype(BF16)
        out[place, tiles] = tile


def prepare(groups, tiles, kinds, diag_table, pre_table, residual, image, sent, precond, diagonal):
    held = tiles // groups
    rows = groups * GROUP
    shape = (groups, GROUP, LANES)
    dots = [None] * 3
    for block in range(held):
        kind = kinds[block]
        left = residual[block]
        value = jnp.dot(
            left.reshape(rows, LANES), pre_table[kind],
            precision=lax.Precision.HIGHEST, preferred_element_type=F32,
        )
        scaled = jnp.dot(
            value, diag_table[kind],
            precision=lax.Precision.HIGHEST, preferred_element_type=F32,
        ).reshape(shape)
        value = value.reshape(shape)
        precond[block] = value
        diagonal[block] = scaled
        for place in range(sent.shape[0]):
            sent[place, block * groups : (block + 1) * groups] = value.astype(BF16)
        terms = [left * value, value * scaled]
        if image is not None:
            terms.append(value * image[block])
        for kind, term in enumerate(terms):
            dots[kind] = term if dots[kind] is None else dots[kind] + term
    columns = {}
    for kind, dot in enumerate(dots):
        if dot is not None:
            for group in range(groups):
                columns[group, kind] = jnp.sum(dot[group], axis=1, keepdims=True)
    tile = in_parts(in_tile(columns))
    for place in range(sent.shape[0]):
        sent[place, tiles] = tile


def begin(groups, tiles, kinds, diag_table, pre_table, residual, sent, precond, diagonal):
    prepare(
        groups, tiles, kinds, diag_table, pre_table, residual, None, sent, precond, diagonal
    )


def update(groups, tiles, more, kinds, diag_table, pre_table, arrived, totals, carry, *refs):
    precond, diagonal, direction, image, answer, residual = refs[:6]
    if more:
        sent, new_carry, new_precond, new_diagonal = refs[6:10]
        new_direction, new_image, new_answer, new_residual = refs[10:]
    else:
        new_answer, new_residual = refs[6:]
    held = tiles // groups
    depth = arrived.shape[0]
    energies = whole(total_of([(arrived, (place, tiles)) for place in range(depth)]))
    sums, before = totals[...], carry[...]
    columns = {}
    for group in range(groups):

        def column(tile, kind):
            lane = group * KEYS + 3 * kind
            return tile[:, lane : lane + 1]

        now = column(sums, 0)
        beta = now / column(before, 0)
        bent = column(energies, 0) + column(sums, 1)
        bent = bent + 2.0 * beta * column(sums, 2) + beta * beta * column(before, 1)
        step = now / bent
        columns[group, 0], columns[group, 1] = now, bent
        for block in range(held):
            tile = block * groups + group
            applied = total_of([(arrived, (place, tile)) for place in range(depth)])
            applied = applied + diagonal[block, group]
            heading = precond[block, group] + beta * direction[block, group]
            applied = applied + beta * image[block, group]
            if more:
                new_direction[block, group] = heading
                new_image[block, group] = applied
            new_answer[block, group] = answer[block, group] + step * heading
            new_residual[block, group] = residual[block, group] - step * applied
    if more:
        new_carry[...] = in_tile(columns)
        prepare(
            groups, tiles, kinds, diag_table, pre_table, new_residual, new_image,
            sent, new_precond, new_diagonal,
        )


def call(body, shapes, operands, smem, name, flops, scratch=(), aliases={}):
    return pl.pallas_call(
        body,
        out_shape=shapes,
        in_specs=[SMEM] * smem + [VMEM] * (len(operands) - smem),
        out_specs=jax.tree.map(lambda _: VMEM, shapes),
        scratch_shapes=list(scratch),
        input_output_aliases=dict(aliases),
        compiler_params=pltpu.CompilerParams(vmem_limit_bytes=32 * 1024 * 1024),
        cost_estimate=pl.CostEstimate(flops=flops, bytes_accessed=1 << 20, transcendentals=0),
        name=name,
    )(*operands)


def per_device(right_side, jacobians, week_blocks, block_kind, diagonal_table, precond_table):
    rhs_all = right_side.shape[0]
    rows = rhs_all // 2
    groups = rows // GROUP
    week_count, rank_count, columns = jacobians.shape
    picks = 2 * week_blocks.shape[1]
    own_blocks = right_side.shape[2] // LANES
    z_size, y_size, x_size = (lax.axis_size(axis) for axis in (Z, Y, X))
    here_y = lax.axis_index(Y)
    core = lax.axis_index(CORE)
    held = 2 * own_blocks
    tiles = held * groups
    shape = jax.ShapeDtypeStruct

    other_jacobians = shifted(jacobians, CORE, 1)
    other_kind = shifted(block_kind, CORE, 1)
    other_ids = shifted(week_blocks, CORE, 1)
    right = right_side[:, 0, :].reshape(2, rows, own_blocks, LANES)
    right = jnp.transpose(right, (0, 2, 1, 3))
    kept = jnp.where(core == 0, right[0], right[1])
    given = jnp.where(core == 0, right[1], right[0])
    right = jnp.concatenate([kept, shifted(given, CORE, 1)])
    right = right.reshape(held, groups, GROUP, LANES)
    kinds = jnp.concatenate([block_kind, other_kind], axis=1).reshape(-1)

    vector = shape((held, groups, GROUP, LANES), F32)
    tile = shape((GROUP, LANES), F32)
    sent_shape = shape((z_size, tiles + 1, GROUP, LANES), BF16)
    term_shape = shape((z_size * tiles + 1, GROUP, LANES), BF16)
    part_shape = shape((week_count * rank_count // LANES * groups + 1, GROUP, LANES), BF16)
    big_flops = 2 * week_count * rank_count * columns * 2 * rows
    slots = y_size * z_size * held
    tables = (kinds, diagonal_table, precond_table)

    sent, precond, diagonal = call(
        functools.partial(begin, groups, tiles),
        (sent_shape, vector, vector),
        (*tables, right),
        1, "begin", 1 << 22,
    )
    ids = jnp.stack([week_blocks, other_ids], axis=1)
    owner = ids // own_blocks
    place = ids % own_blocks + own_blocks * jnp.arange(2, dtype=jnp.int32)[None, :, None]
    owner_z, owner_y = owner // y_size, owner % y_size
    pick_at = ((here_y - owner_y) % y_size) * z_size + owner_z
    pick_at = (pick_at * (tiles + 1) + place * groups).reshape(-1)
    put_at = ((((owner_y - here_y) % y_size) * z_size + owner_z) * held + place).reshape(-1)

    def operate(sent):
        along_z = exchange(sent, Z)
        got = jnp.concatenate(from_ring(along_z, Y)).reshape(-1, GROUP, LANES)
        partial = call(
            functools.partial(project, groups, tiles, picks),
            part_shape,
            (pick_at, got, jacobians, other_jacobians),
            1, "project", big_flops,
        )
        own = shape(term_shape.shape, F32)
        *terms, totals = call(
            functools.partial(spread, groups, tiles, picks),
            (own, *[term_shape] * (y_size - 1), tile),
            (put_at, *from_ring(partial, X), jacobians, other_jacobians),
            1, "spread", big_flops,
            scratch=[pltpu.VMEM((slots, groups, GROUP, LANES), F32)],
        )
        for k in by_distance(y_size):
            terms[k] = shifted(terms[k], Y, k)
        summed = call(
            functools.partial(add_up, groups, tiles), sent_shape, tuple(terms), 0, "add_up", 1 << 20
        )
        return exchange(summed, Z), totals

    zeros = jnp.zeros(vector.shape, F32)
    carry = jnp.full(tile.shape, jnp.inf, F32)
    carry = jnp.where(jnp.arange(LANES)[None, :] % KEYS == 0, carry, 0.0)
    state = (sent, carry, precond, diagonal, zeros, zeros, zeros, right)

    def advance(state, more):
        sent, carry, *vectors = state
        arrived, totals = operate(sent)
        shapes, aliases = (vector, vector), {}
        if more:
            shapes = (sent_shape, tile, *[vector] * 6)
            aliases = {5 + place: 1 + place for place in range(7)}
        return tuple(
            call(
                functools.partial(update, groups, tiles, more),
                shapes,
                (*tables, arrived, totals, carry, *vectors),
                1, "update", 1 << 22, aliases=aliases,
            )
        )

    def turn(carried):
        step, state = carried
        step, state = lax.optimization_barrier((step + 1, state))
        return step, advance(state, True)

    carried = (jnp.int32(0), state)
    state = lax.while_loop(lambda now: now[0] < ITERS, turn, carried)[1]
    answer, residual = state[-2:]

    results = jnp.stack([answer, residual]).reshape(2, held, rows, LANES)
    other = shifted(results[:, own_blocks:], CORE, 1)
    own = results[:, :own_blocks]
    first = jnp.where(core == 0, own, other)
    second = jnp.where(core == 0, other, own)
    results = jnp.stack([first, second], axis=1)
    results = jnp.transpose(results, (0, 1, 3, 2, 4)).reshape(2, rhs_all, 1, -1)
    return (results[0], results[1])


def solution(mesh):
    torus = Mesh(mesh.devices.reshape(8, 4, 4, 2), ("week_0", "week_1", "seg_0", "seg_1"))
    return jax.shard_map(
        per_device,
        mesh=torus,
        in_specs=(P(None, SEG, WEEK), P(WEEK, None, SEG), P(WEEK, SEG), P(SEG, WEEK), P(), P()),
        out_specs=(P(None, SEG, WEEK), P(None, SEG, WEEK)),
        check_vma=False,
    )
```

```python
import functools

import jax
import jax.numpy as jnp
from jax import lax
from jax.experimental import pallas as pl
from jax.experimental.pallas import tpu as pltpu
from jax.sharding import Mesh
from jax.sharding import PartitionSpec as P

ITERS = 4
SEG = ("seg_0", "seg_1")
WEEK = ("week_0", "week_1")
Z, Y, X, CORE = "week_0", "week_1", "seg_0", "seg_1"
BF16 = jnp.bfloat16
F32 = jnp.float32
LANES = 128
GROUP = 8
KEYS = 16
VMEM = pl.BlockSpec(memory_space=pltpu.VMEM)
SMEM = pl.BlockSpec(memory_space=pltpu.SMEM)


def ring(axis, shift):
    size = lax.axis_size(axis)
    return [(place, (place + shift) % size) for place in range(size)]


def shifted(array, axis, shift):
    return lax.ppermute(array, axis, ring(axis, shift))


def by_distance(size):
    return sorted(range(1, size), key=lambda k: (min(k, size - k), k))


def from_ring(array, axis):
    size = lax.axis_size(axis)
    moved = {0: array}
    for k in by_distance(size):
        moved[k] = shifted(array, axis, k)
    return [moved[k] for k in range(size)]


def exchange(array, axis):
    return lax.all_to_all(array, axis, 0, 0, tiled=True)


def lanes():
    return lax.broadcasted_iota(jnp.int32, (GROUP, LANES), 1)


def whole(tile):
    return tile + pltpu.roll(tile, LANES - 1, 1) + pltpu.roll(tile, LANES - 2, 1)


def in_parts(values):
    high = values.astype(BF16).astype(F32)
    rest = values - high
    middle = rest.astype(BF16).astype(F32)
    return (high + pltpu.roll(middle, 1, 1) + pltpu.roll(rest - middle, 2, 1)).astype(BF16)


def firsts(tile, kinds, groups):
    lane = lanes()
    keep = (lane % KEYS % 3 == 0) & (lane % KEYS < 3 * kinds) & (lane < groups * KEYS)
    return jnp.where(keep, tile, 0.0)


def in_tile(columns):
    lane = lanes()
    tile = jnp.zeros((GROUP, LANES), F32)
    for (group, kind), column in columns.items():
        tile = jnp.where(lane == group * KEYS + 3 * kind, column, tile)
    return tile


def total_of(refs_and_places):
    total = None
    for ref, place in refs_and_places:
        value = ref[place].astype(F32)
        total = value if total is None else total + value
    return total


def project(groups, tiles, picks, at_ref, got, near, far, out):
    weeks, rank, columns = near.shape
    rows = groups * GROUP
    each = picks // 2
    for week in range(weeks):
        total = None
        for side, factor in enumerate((near, far)):
            blocks = []
            for pick in range(each):
                number = week * picks + side * each + pick
                block = got[pl.ds(at_ref[number], groups)]
                blocks.append(block.astype(F32).reshape(rows, LANES).astype(BF16))
            term = lax.dot_general(
                jnp.concatenate(blocks, axis=1),
                factor[week],
                (((1,), (1,)), ((), ())),
                preferred_element_type=F32,
            )
            total = term if total is None else total + term
        for half in range(rank // LANES):
            piece = total[:, half * LANES : (half + 1) * LANES].reshape(groups, GROUP, LANES)
            first = (week * (rank // LANES) + half) * groups
            out[first : first + groups] = piece.astype(BF16)
    sums = total_of([(got, place) for place in range(tiles, got.shape[0], tiles + 1)])
    out[out.shape[0] - 1] = in_parts(firsts(whole(sums), 3, groups))


def spread(groups, tiles, picks, at_ref, *refs):
    count = len(refs) // 2 - 2
    parts, (near, far) = refs[:count], refs[count : count + 2]
    outs, totals, sums = refs[count + 2 : 2 * count + 2], refs[-2], refs[-1]
    weeks, rank, columns = near.shape
    rows = groups * GROUP
    each = picks // 2
    halves = rank // LANES
    last = parts[0].shape[0] - 1
    totals[...] = firsts(whole(total_of([(part, last) for part in parts])), 3, groups)
    sums[...] = jnp.zeros_like(sums)
    energy = jnp.zeros((groups, GROUP, LANES), F32)
    for week in range(weeks):
        pieces = []
        for half in range(halves):
            first = (week * halves + half) * groups
            piece = total_of([(part, slice(first, first + groups)) for part in parts])
            energy = energy + piece * piece
            pieces.append(piece.reshape(rows, LANES).astype(BF16))
        projected = jnp.concatenate(pieces, axis=1)
        for side, factor in enumerate((near, far)):
            term = jnp.dot(projected, factor[week], preferred_element_type=F32)
            for pick in range(each):
                place = at_ref[week * picks + side * each + pick]
                block = term[:, pick * LANES : (pick + 1) * LANES]
                sums[place] = sums[place] + block.reshape(groups, GROUP, LANES)
    columns = {}
    for group in range(groups):
        columns[group, 0] = jnp.sum(energy[group], axis=1, keepdims=True)
    tile = in_parts(in_tile(columns))
    blocks = outs[0].shape[0] // groups
    for k, out in enumerate(outs):
        for block in range(blocks):
            value = sums[k * blocks + block]
            out[block * groups : (block + 1) * groups] = value.astype(out.dtype)
        out[blocks * groups] = tile.astype(out.dtype)


def add_up(groups, tiles, *refs):
    arrived, out = refs[:-1], refs[-1]
    depth = out.shape[0]
    sums = total_of([(ref, depth * tiles) for ref in arrived])
    tile = in_parts(firsts(whole(sums), 1, groups))
    for place in range(depth):
        span = slice(place * tiles, (place + 1) * tiles)
        out[place, 0:tiles] = total_of([(ref, span) for ref in arrived]).astype(BF16)
        out[place, tiles] = tile


def prepare(groups, tiles, sides, diag_table, pre_table, residual, image, sent, precond, diagonal):
    held = tiles // groups
    own = held // 2
    rows = groups * GROUP
    shape = (groups, GROUP, LANES)
    dots = [None] * 3
    for block in range(held):
        kind = sides[block // own][0, block % own]
        left = residual[block]
        value = jnp.dot(
            left.reshape(rows, LANES), pre_table[kind],
            precision=lax.Precision.HIGHEST, preferred_element_type=F32,
        )
        scaled = jnp.dot(
            value, diag_table[kind],
            precision=lax.Precision.HIGHEST, preferred_element_type=F32,
        ).reshape(shape)
        value = value.reshape(shape)
        precond[block] = value
        diagonal[block] = scaled
        for place in range(sent.shape[0]):
            sent[place, block * groups : (block + 1) * groups] = value.astype(BF16)
        terms = [left * value, value * scaled]
        if image is not None:
            terms.append(value * image[block])
        for kind, term in enumerate(terms):
            dots[kind] = term if dots[kind] is None else dots[kind] + term
    columns = {}
    for kind, dot in enumerate(dots):
        if dot is not None:
            for group in range(groups):
                columns[group, kind] = jnp.sum(dot[group], axis=1, keepdims=True)
    tile = in_parts(in_tile(columns))
    for place in range(sent.shape[0]):
        sent[place, tiles] = tile


def begin(groups, tiles, near_kinds, far_kinds, diag_table, pre_table, residual, sent, precond, diagonal):
    sides = (near_kinds, far_kinds)
    prepare(
        groups, tiles, sides, diag_table, pre_table, residual, None, sent, precond, diagonal
    )


def update(groups, tiles, more, near_kinds, far_kinds, diag_table, pre_table, *refs):
    arrived, totals, carry, *refs = refs
    precond, diagonal, direction, image, answer, residual = refs[:6]
    if more:
        sent, new_carry, new_precond, new_diagonal = refs[6:10]
        new_direction, new_image, new_answer, new_residual = refs[10:]
    else:
        new_answer, new_residual = refs[6:]
    held = tiles // groups
    depth = arrived.shape[0]
    energies = whole(total_of([(arrived, (place, tiles)) for place in range(depth)]))
    sums, before = totals[...], carry[...]
    columns = {}
    for group in range(groups):

        def column(tile, kind):
            lane = group * KEYS + 3 * kind
            return tile[:, lane : lane + 1]

        now = column(sums, 0)
        beta = now / column(before, 0)
        bent = column(energies, 0) + column(sums, 1)
        bent = bent + 2.0 * beta * column(sums, 2) + beta * beta * column(before, 1)
        step = now / bent
        columns[group, 0], columns[group, 1] = now, bent
        for block in range(held):
            tile = block * groups + group
            applied = total_of([(arrived, (place, tile)) for place in range(depth)])
            applied = applied + diagonal[block, group]
            heading = precond[block, group] + beta * direction[block, group]
            applied = applied + beta * image[block, group]
            if more:
                new_direction[block, group] = heading
                new_image[block, group] = applied
            new_answer[block, group] = answer[block, group] + step * heading
            new_residual[block, group] = residual[block, group] - step * applied
    if more:
        new_carry[...] = in_tile(columns)
        prepare(
            groups, tiles, (near_kinds, far_kinds), diag_table, pre_table, new_residual, new_image,
            sent, new_precond, new_diagonal,
        )


def call(body, shapes, operands, smem, name, flops, scratch=(), aliases={}):
    return pl.pallas_call(
        body,
        out_shape=shapes,
        in_specs=[SMEM] * smem + [VMEM] * (len(operands) - smem),
        out_specs=jax.tree.map(lambda _: VMEM, shapes),
        scratch_shapes=list(scratch),
        input_output_aliases=dict(aliases),
        compiler_params=pltpu.CompilerParams(vmem_limit_bytes=32 * 1024 * 1024),
        cost_estimate=pl.CostEstimate(flops=flops, bytes_accessed=1 << 20, transcendentals=0),
        name=name,
    )(*operands)


def per_device(right_side, jacobians, week_blocks, block_kind, diagonal_table, precond_table):
    rhs_all = right_side.shape[0]
    rows = rhs_all // 2
    groups = rows // GROUP
    week_count, rank_count, columns = jacobians.shape
    picks = 2 * week_blocks.shape[1]
    own_blocks = right_side.shape[2] // LANES
    z_size, y_size, x_size = (lax.axis_size(axis) for axis in (Z, Y, X))
    here_y = lax.axis_index(Y)
    core = lax.axis_index(CORE)
    held = 2 * own_blocks
    tiles = held * groups
    shape = jax.ShapeDtypeStruct

    other_kind = shifted(block_kind, CORE, 1)
    other_ids = shifted(week_blocks, CORE, 1)
    right = right_side[:, 0, :].reshape(2, rows, own_blocks, LANES)
    right = jnp.transpose(right, (0, 2, 1, 3))
    kept = jnp.where(core == 0, right[0], right[1])
    given = jnp.where(core == 0, right[1], right[0])
    received = shifted(given, CORE, 1)
    received, other_kind, other_ids, later = lax.optimization_barrier(
        (received, other_kind, other_ids, jacobians)
    )
    other_jacobians = shifted(later, CORE, 1)
    right = jnp.concatenate([kept, received])
    right = right.reshape(held, groups, GROUP, LANES)

    vector = shape((held, groups, GROUP, LANES), F32)
    tile = shape((GROUP, LANES), F32)
    sent_shape = shape((z_size, tiles + 1, GROUP, LANES), BF16)
    term_shape = shape((z_size * tiles + 1, GROUP, LANES), BF16)
    part_shape = shape((week_count * rank_count // LANES * groups + 1, GROUP, LANES), BF16)
    big_flops = 2 * week_count * rank_count * columns * 2 * rows
    slots = y_size * z_size * held
    tables = (block_kind, other_kind, diagonal_table, precond_table)

    sent, precond, diagonal = call(
        functools.partial(begin, groups, tiles),
        (sent_shape, vector, vector),
        (*tables, right),
        2, "begin", 1 << 22,
    )
    ids = jnp.stack([week_blocks, other_ids], axis=1)
    owner = ids // own_blocks
    place = ids % own_blocks + own_blocks * jnp.arange(2, dtype=jnp.int32)[None, :, None]
    owner_z, owner_y = owner // y_size, owner % y_size
    pick_at = ((here_y - owner_y) % y_size) * z_size + owner_z
    pick_at = (pick_at * (tiles + 1) + place * groups).reshape(-1)
    put_at = ((((owner_y - here_y) % y_size) * z_size + owner_z) * held + place).reshape(-1)

    def operate(sent):
        along_z = exchange(sent, Z)
        got = jnp.concatenate(from_ring(along_z, Y)).reshape(-1, GROUP, LANES)
        partial = call(
            functools.partial(project, groups, tiles, picks),
            part_shape,
            (pick_at, got, jacobians, other_jacobians),
            1, "project", big_flops,
        )
        own = shape(term_shape.shape, F32)
        *terms, totals = call(
            functools.partial(spread, groups, tiles, picks),
            (own, *[term_shape] * (y_size - 1), tile),
            (put_at, *from_ring(partial, X), jacobians, other_jacobians),
            1, "spread", big_flops,
            scratch=[pltpu.VMEM((slots, groups, GROUP, LANES), F32)],
        )
        for k in by_distance(y_size):
            terms[k] = shifted(terms[k], Y, k)
        summed = call(
            functools.partial(add_up, groups, tiles), sent_shape, tuple(terms), 0, "add_up", 1 << 20
        )
        return exchange(summed, Z), totals

    zeros = jnp.zeros(vector.shape, F32)
    carry = jnp.full(tile.shape, jnp.inf, F32)
    carry = jnp.where(jnp.arange(LANES)[None, :] % KEYS == 0, carry, 0.0)
    state = (sent, carry, precond, diagonal, zeros, zeros, zeros, right)

    def advance(state, more):
        sent, carry, *vectors = state
        arrived, totals = operate(sent)
        shapes, aliases = (vector, vector), {}
        if more:
            shapes = (sent_shape, tile, *[vector] * 6)
            aliases = {6 + place: 1 + place for place in range(7)}
        return tuple(
            call(
                functools.partial(update, groups, tiles, more),
                shapes,
                (*tables, arrived, totals, carry, *vectors),
                2, "update", 1 << 22, aliases=aliases,
            )
        )

    def turn(carried):
        step, state = carried
        step, state = lax.optimization_barrier((step + 1, state))
        return step, advance(state, True)

    carried = (jnp.int32(0), state)
    state = lax.while_loop(lambda now: now[0] < ITERS, turn, carried)[1]
    answer, residual = state[-2:]

    results = jnp.stack([answer, residual]).reshape(2, held, rows, LANES)
    other = shifted(results[:, own_blocks:], CORE, 1)
    own = results[:, :own_blocks]
    first = jnp.where(core == 0, own, other)
    second = jnp.where(core == 0, other, own)
    results = jnp.stack([first, second], axis=1)
    results = jnp.transpose(results, (0, 1, 3, 2, 4)).reshape(2, rhs_all, 1, -1)
    return (results[0], results[1])


def solution(mesh):
    torus = Mesh(mesh.devices.reshape(8, 4, 4, 2), ("week_0", "week_1", "seg_0", "seg_1"))
    return jax.shard_map(
        per_device,
        mesh=torus,
        in_specs=(P(None, SEG, WEEK), P(WEEK, None, SEG), P(WEEK, SEG), P(SEG, WEEK), P(), P()),
        out_specs=(P(None, SEG, WEEK), P(None, SEG, WEEK)),
        check_vma=False,
    )
```

```python
import functools

import jax
import jax.numpy as jnp
from jax import lax
from jax.experimental import pallas as pl
from jax.experimental.pallas import tpu as pltpu
from jax.sharding import Mesh
from jax.sharding import PartitionSpec as P

ITERS = 4
SEG = ("seg_0", "seg_1")
WEEK = ("week_0", "week_1")
Z, Y, X, CORE = "week_0", "week_1", "seg_0", "seg_1"
BF16 = jnp.bfloat16
F32 = jnp.float32
LANES = 128
GROUP = 8
KEYS = 16
VMEM = pl.BlockSpec(memory_space=pltpu.VMEM)
SMEM = pl.BlockSpec(memory_space=pltpu.SMEM)


def ring(axis, shift):
    size = lax.axis_size(axis)
    return [(place, (place + shift) % size) for place in range(size)]


def shifted(array, axis, shift):
    return lax.ppermute(array, axis, ring(axis, shift))


def by_distance(size):
    return sorted(range(1, size), key=lambda k: (min(k, size - k), k))


def from_ring(array, axis):
    size = lax.axis_size(axis)
    moved = {0: array}
    for k in by_distance(size):
        moved[k] = shifted(array, axis, k)
    return [moved[k] for k in range(size)]


def exchange(array, axis):
    return lax.all_to_all(array, axis, 0, 0, tiled=True)


def lanes():
    return lax.broadcasted_iota(jnp.int32, (GROUP, LANES), 1)


def whole(tile):
    return tile + pltpu.roll(tile, LANES - 1, 1) + pltpu.roll(tile, LANES - 2, 1)


def in_parts(values):
    high = values.astype(BF16).astype(F32)
    rest = values - high
    middle = rest.astype(BF16).astype(F32)
    return (high + pltpu.roll(middle, 1, 1) + pltpu.roll(rest - middle, 2, 1)).astype(BF16)


def firsts(tile, kinds, groups):
    lane = lanes()
    keep = (lane % KEYS % 3 == 0) & (lane % KEYS < 3 * kinds) & (lane < groups * KEYS)
    return jnp.where(keep, tile, 0.0)


def in_tile(columns):
    lane = lanes()
    tile = jnp.zeros((GROUP, LANES), F32)
    for (group, kind), column in columns.items():
        tile = jnp.where(lane == group * KEYS + 3 * kind, column, tile)
    return tile


def total_of(refs_and_places):
    total = None
    for ref, place in refs_and_places:
        value = ref[place].astype(F32)
        total = value if total is None else total + value
    return total


def project(groups, tiles, picks, at_ref, got, near, far, out):
    weeks, rank, columns = near.shape
    rows = groups * GROUP
    each = picks // 2
    for week in range(weeks):
        total = None
        for side, factor in enumerate((near, far)):
            blocks = []
            for pick in range(each):
                number = week * picks + side * each + pick
                block = got[pl.ds(at_ref[number], groups)]
                blocks.append(block.astype(F32).reshape(rows, LANES).astype(BF16))
            term = lax.dot_general(
                jnp.concatenate(blocks, axis=1),
                factor[week],
                (((1,), (1,)), ((), ())),
                preferred_element_type=F32,
            )
            total = term if total is None else total + term
        for half in range(rank // LANES):
            piece = total[:, half * LANES : (half + 1) * LANES].reshape(groups, GROUP, LANES)
            first = (week * (rank // LANES) + half) * groups
            out[first : first + groups] = piece.astype(BF16)
    sums = total_of([(got, place) for place in range(tiles, got.shape[0], tiles + 1)])
    out[out.shape[0] - 1] = in_parts(firsts(whole(sums), 3, groups))


def spread(groups, tiles, picks, at_ref, *refs):
    count = len(refs) // 2 - 2
    parts, (near, far) = refs[:count], refs[count : count + 2]
    outs, totals, sums = refs[count + 2 : 2 * count + 2], refs[-2], refs[-1]
    weeks, rank, columns = near.shape
    rows = groups * GROUP
    each = picks // 2
    halves = rank // LANES
    last = parts[0].shape[0] - 1
    totals[...] = firsts(whole(total_of([(part, last) for part in parts])), 3, groups)
    sums[...] = jnp.zeros_like(sums)
    energy = jnp.zeros((groups, GROUP, LANES), F32)
    for week in range(weeks):
        pieces = []
        for half in range(halves):
            first = (week * halves + half) * groups
            piece = total_of([(part, slice(first, first + groups)) for part in parts])
            energy = energy + piece * piece
            pieces.append(piece.reshape(rows, LANES).astype(BF16))
        projected = jnp.concatenate(pieces, axis=1)
        for side, factor in enumerate((near, far)):
            term = jnp.dot(projected, factor[week], preferred_element_type=F32)
            for pick in range(each):
                place = at_ref[week * picks + side * each + pick]
                block = term[:, pick * LANES : (pick + 1) * LANES]
                sums[place] = sums[place] + block.reshape(groups, GROUP, LANES)
    columns = {}
    for group in range(groups):
        columns[group, 0] = jnp.sum(energy[group], axis=1, keepdims=True)
    tile = in_parts(in_tile(columns))
    blocks = outs[0].shape[0] // groups
    for k, out in enumerate(outs):
        for block in range(blocks):
            value = sums[k * blocks + block]
            out[block * groups : (block + 1) * groups] = value.astype(out.dtype)
        out[blocks * groups] = tile.astype(out.dtype)


def add_up(groups, tiles, *refs):
    arrived, out = refs[:-1], refs[-1]
    depth = out.shape[0]
    sums = total_of([(ref, depth * tiles) for ref in arrived])
    tile = in_parts(firsts(whole(sums), 1, groups))
    for place in range(depth):
        span = slice(place * tiles, (place + 1) * tiles)
        out[place, 0:tiles] = total_of([(ref, span) for ref in arrived]).astype(BF16)
        out[place, tiles] = tile


def prepare(groups, tiles, sides, diag_table, pre_table, residual, image, sent, precond, diagonal):
    held = tiles // groups
    own = held // 2
    rows = groups * GROUP
    shape = (groups, GROUP, LANES)
    dots = [None] * 3
    for block in range(held):
        kind = sides[block // own][0, block % own]
        left = residual[block]
        value = jnp.dot(
            left.reshape(rows, LANES), pre_table[kind],
            precision=lax.Precision.HIGHEST, preferred_element_type=F32,
        )
        scaled = jnp.dot(
            value, diag_table[kind],
            precision=lax.Precision.HIGHEST, preferred_element_type=F32,
        ).reshape(shape)
        value = value.reshape(shape)
        precond[block] = value
        diagonal[block] = scaled
        for place in range(sent.shape[0]):
            sent[place, block * groups : (block + 1) * groups] = value.astype(BF16)
        terms = [left * value, value * scaled]
        if image is not None:
            terms.append(value * image[block])
        for kind, term in enumerate(terms):
            dots[kind] = term if dots[kind] is None else dots[kind] + term
    columns = {}
    for kind, dot in enumerate(dots):
        if dot is not None:
            for group in range(groups):
                columns[group, kind] = jnp.sum(dot[group], axis=1, keepdims=True)
    tile = in_parts(in_tile(columns))
    for place in range(sent.shape[0]):
        sent[place, tiles] = tile


def begin(groups, tiles, near_kinds, far_kinds, diag_table, pre_table, residual, sent, precond, diagonal):
    sides = (near_kinds, far_kinds)
    prepare(
        groups, tiles, sides, diag_table, pre_table, residual, None, sent, precond, diagonal
    )


def update(groups, tiles, more, near_kinds, far_kinds, diag_table, pre_table, *refs):
    arrived, totals, carry, *refs = refs
    precond, diagonal, direction, image, answer, residual = refs[:6]
    if more:
        sent, new_carry, new_precond, new_diagonal = refs[6:10]
        new_direction, new_image, new_answer, new_residual = refs[10:]
    else:
        new_answer, new_residual = refs[6:]
    held = tiles // groups
    depth = arrived.shape[0]
    energies = whole(total_of([(arrived, (place, tiles)) for place in range(depth)]))
    sums, before = totals[...], carry[...]
    columns = {}
    for group in range(groups):

        def column(tile, kind):
            lane = group * KEYS + 3 * kind
            return tile[:, lane : lane + 1]

        now = column(sums, 0)
        beta = now / column(before, 0)
        bent = column(energies, 0) + column(sums, 1)
        bent = bent + 2.0 * beta * column(sums, 2) + beta * beta * column(before, 1)
        step = now / bent
        columns[group, 0], columns[group, 1] = now, bent
        for block in range(held):
            tile = block * groups + group
            applied = total_of([(arrived, (place, tile)) for place in range(depth)])
            applied = applied + diagonal[block, group]
            heading = precond[block, group] + beta * direction[block, group]
            applied = applied + beta * image[block, group]
            if more:
                new_direction[block, group] = heading
                new_image[block, group] = applied
            new_answer[block, group] = answer[block, group] + step * heading
            new_residual[block, group] = residual[block, group] - step * applied
    if more:
        new_carry[...] = in_tile(columns)
        prepare(
            groups, tiles, (near_kinds, far_kinds), diag_table, pre_table, new_residual, new_image,
            sent, new_precond, new_diagonal,
        )


def call(body, shapes, operands, smem, name, flops, scratch=(), aliases={}):
    return pl.pallas_call(
        body,
        out_shape=shapes,
        in_specs=[SMEM] * smem + [VMEM] * (len(operands) - smem),
        out_specs=jax.tree.map(lambda _: VMEM, shapes),
        scratch_shapes=list(scratch),
        input_output_aliases=dict(aliases),
        compiler_params=pltpu.CompilerParams(vmem_limit_bytes=32 * 1024 * 1024),
        cost_estimate=pl.CostEstimate(flops=flops, bytes_accessed=1 << 20, transcendentals=0),
        name=name,
    )(*operands)


def per_device(right_side, jacobians, week_blocks, block_kind, diagonal_table, precond_table):
    rhs_all = right_side.shape[0]
    rows = rhs_all // 2
    groups = rows // GROUP
    week_count, rank_count, columns = jacobians.shape
    picks = 2 * week_blocks.shape[1]
    own_blocks = right_side.shape[2] // LANES
    z_size, y_size, x_size = (lax.axis_size(axis) for axis in (Z, Y, X))
    here_y = lax.axis_index(Y)
    core = lax.axis_index(CORE)
    held = 2 * own_blocks
    tiles = held * groups
    shape = jax.ShapeDtypeStruct

    other_kind = shifted(block_kind, CORE, 1)
    other_ids = shifted(week_blocks, CORE, 1)
    right = right_side[:, 0, :].reshape(2, rows, own_blocks, LANES)
    right = jnp.transpose(right, (0, 2, 1, 3))
    kept = jnp.where(core == 0, right[0], right[1])
    given = jnp.where(core == 0, right[1], right[0])
    received = shifted(given, CORE, 1)
    received, other_kind, other_ids, later = lax.optimization_barrier(
        (received, other_kind, other_ids, jacobians)
    )
    other_jacobians = shifted(later, CORE, 1)
    right = jnp.concatenate([kept, received])
    right = right.reshape(held, groups, GROUP, LANES)

    vector = shape((held, groups, GROUP, LANES), F32)
    tile = shape((GROUP, LANES), F32)
    sent_shape = shape((z_size, tiles + 1, GROUP, LANES), BF16)
    term_shape = shape((z_size * tiles + 1, GROUP, LANES), BF16)
    part_shape = shape((week_count * rank_count // LANES * groups + 1, GROUP, LANES), BF16)
    big_flops = 2 * week_count * rank_count * columns * 2 * rows
    slots = y_size * z_size * held
    tables = (block_kind, other_kind, diagonal_table, precond_table)

    sent, precond, diagonal = call(
        functools.partial(begin, groups, tiles),
        (sent_shape, vector, vector),
        (*tables, right),
        2, "begin", 1 << 22,
    )
    precond, own_ids, other_ids = lax.optimization_barrier((precond, week_blocks, other_ids))
    ids = jnp.stack([own_ids, other_ids], axis=1)
    owner = ids // own_blocks
    place = ids % own_blocks + own_blocks * jnp.arange(2, dtype=jnp.int32)[None, :, None]
    owner_z, owner_y = owner // y_size, owner % y_size
    pick_at = ((here_y - owner_y) % y_size) * z_size + owner_z
    pick_at = (pick_at * (tiles + 1) + place * groups).reshape(-1)
    put_at = ((((owner_y - here_y) % y_size) * z_size + owner_z) * held + place).reshape(-1)

    def operate(sent):
        along_z = exchange(sent, Z)
        got = jnp.concatenate(from_ring(along_z, Y)).reshape(-1, GROUP, LANES)
        partial = call(
            functools.partial(project, groups, tiles, picks),
            part_shape,
            (pick_at, got, jacobians, other_jacobians),
            1, "project", big_flops,
        )
        own = shape(term_shape.shape, F32)
        *terms, totals = call(
            functools.partial(spread, groups, tiles, picks),
            (own, *[term_shape] * (y_size - 1), tile),
            (put_at, *from_ring(partial, X), jacobians, other_jacobians),
            1, "spread", big_flops,
            scratch=[pltpu.VMEM((slots, groups, GROUP, LANES), F32)],
        )
        for k in by_distance(y_size):
            terms[k] = shifted(terms[k], Y, k)
        summed = call(
            functools.partial(add_up, groups, tiles), sent_shape, tuple(terms), 0, "add_up", 1 << 20
        )
        return exchange(summed, Z), totals

    zeros = jnp.zeros(vector.shape, F32)
    carry = jnp.full(tile.shape, jnp.inf, F32)
    carry = jnp.where(jnp.arange(LANES)[None, :] % KEYS == 0, carry, 0.0)
    state = (sent, carry, precond, diagonal, zeros, zeros, zeros, right)

    def advance(state, more):
        sent, carry, *vectors = state
        arrived, totals = operate(sent)
        shapes, aliases = (vector, vector), {}
        if more:
            shapes = (sent_shape, tile, *[vector] * 6)
            aliases = {6 + place: 1 + place for place in range(7)}
        return tuple(
            call(
                functools.partial(update, groups, tiles, more),
                shapes,
                (*tables, arrived, totals, carry, *vectors),
                2, "update", 1 << 22, aliases=aliases,
            )
        )

    def turn(carried):
        step, state = carried
        step, state = lax.optimization_barrier((step + 1, state))
        return step, advance(state, True)

    carried = (jnp.int32(0), state)
    state = lax.while_loop(lambda now: now[0] < ITERS, turn, carried)[1]
    answer, residual = state[-2:]

    results = jnp.stack([answer, residual]).reshape(2, held, rows, LANES)
    other = shifted(results[:, own_blocks:], CORE, 1)
    own = results[:, :own_blocks]
    first = jnp.where(core == 0, own, other)
    second = jnp.where(core == 0, other, own)
    results = jnp.stack([first, second], axis=1)
    results = jnp.transpose(results, (0, 1, 3, 2, 4)).reshape(2, rhs_all, 1, -1)
    return (results[0], results[1])


def solution(mesh):
    torus = Mesh(mesh.devices.reshape(8, 4, 4, 2), ("week_0", "week_1", "seg_0", "seg_1"))
    return jax.shard_map(
        per_device,
        mesh=torus,
        in_specs=(P(None, SEG, WEEK), P(WEEK, None, SEG), P(WEEK, SEG), P(SEG, WEEK), P(), P()),
        out_specs=(P(None, SEG, WEEK), P(None, SEG, WEEK)),
        check_vma=False,
    )
```
